32 devices in a mesh: seq: 8 (over z, x), head: 4 (over y, core).
Axes of the slice: x: 2, y: 2, z: 4, core: 2. Of those that a mesh axis runs over, the one named last changes fastest.
Arguments:
- context: bfloat16 [4, 4096, 1024], P('head', 'seq'), may hold values from -6 to 6
- latents: bfloat16 [4, 1024, 1024], P('head'), may hold values from -6 to 6
- offsets: int32 [4], P('head'), may hold values from 0 to 3072
- query_gain: float32 [1024], replicated, may hold values from 0.1 to 1.9
- key_gain: float32 [1024], replicated, may hold values from 0.1 to 1.9
- layer_gain: float32 [2, 1024], replicated, may hold values from 0.1 to 1.9
- cross_query: bfloat16 [1024, 1024], P(('seq', 'head')), may hold values from -0.25 to 0.25
- cross_key: bfloat16 [1024, 1024], P(('seq', 'head')), may hold values from -0.25 to 0.25
- cross_value: bfloat16 [1024, 1024], P(('seq', 'head')), may hold values from -0.1875 to 0.1875
- cross_out: bfloat16 [1024, 1024], P(('seq', 'head')), may hold values from -0.1875 to 0.1875
- layer_qkv: bfloat16 [2, 1024, 3072], P(None, ('seq', 'head')), may hold values from -0.25 to 0.25
- layer_out: bfloat16 [2, 1024, 1024], P(None, ('seq', 'head')), may hold values from -0.1875 to 0.1875
Outputs:
- latent_out: bfloat16 [4, 1024, 1024], P('head', 'seq')
The draws below stay inside these ranges and needn't reach their ends.
Inputs may be any that keep to these rules, and one draw needn't show every extreme that they name: Latent i of row b stands at context position offsets[b] + i.
All inputs are finite; a program needn't handle non-finite values.
Results may differ from the reference program's by a relative error of at most 0.013.
Values may be sent and summed in bfloat16 or wider, within the bound.
No kernel may reach another device: no remote copies, remote signals or barrier semaphores. Data moves between devices by JAX's collectives and lax.ppermute only.
A program may use at most 128 MiB of HBM per device.

```python
import jax
import jax.numpy as jnp
from jax import lax

D = 1024
H = 16
LATENTS = 1024
LAYERS = 2
CTX_DEV = 512
B = 4
L = 4096
N_SEQ = 8


def drawn_rows(key, salt, rows):
    return jnp.clip(jax.random.normal(jax.random.fold_in(key, salt), (B, rows, D), jnp.float32), -6.0, 6.0)


def drawn_weight(key, salt, shape):
    return jnp.clip(jax.random.normal(jax.random.fold_in(key, salt), shape, jnp.float32), -6.0, 6.0) * D ** (-0.5)


def draw_context(key, part):
    value_matrix = drawn_rows(key, 11, L)
    return value_matrix.astype(jnp.bfloat16)


def draw_latents(key, part):
    value_matrix = drawn_rows(key, 21, LATENTS)
    return value_matrix.astype(jnp.bfloat16)


def drawn_cross(key, salt):
    weight = drawn_weight(key, salt, (D, D))
    return weight.astype(jnp.bfloat16)


def draw_cross_query(key, part):
    return drawn_cross(key, 31)


def draw_cross_key(key, part):
    return drawn_cross(key, 32)


def draw_layer_qkv(key, part):
    weight = drawn_weight(key, 33, (LAYERS, D, 3 * D))
    return weight.astype(jnp.bfloat16)


def place_ends(entries, own_key, low, largest):
    shape = entries.shape
    spot = [jax.random.randint(jax.random.fold_in(own_key, axis), (), 0, shape[axis]) for axis in range(len(shape))]
    entries = entries.at[tuple(spot)].set(low)
    longest = shape.index(max(shape))
    spot[longest] = (spot[longest] + 1) % shape[longest]
    return entries.at[tuple(spot)].set(largest)


def steps_of(own_key, extent, cuts, smallest, largest):
    def one(position, blocks):
        steps = jax.random.uniform(jax.random.fold_in(jax.random.fold_in(own_key, 6), position), (blocks,), jnp.float32, smallest / len(cuts), largest / len(cuts))
        return jnp.repeat(jnp.exp(steps), extent[position] // blocks).reshape((-1,) + (1,) * (len(extent) - position - 1))

    factor_of = one(*cuts[0])
    for cut in cuts[1:]:
        factor_of = factor_of * one(*cut)
    return factor_of


def scatter_about(rng, extent, scale, most, split=(), held_as=jnp.bfloat16):
    values = jax.random.normal(rng, extent, jnp.float32) * scale
    if len(split) > 0:
        values = steps_of(rng, extent, split, -0.22, 0.18) * values
    return jnp.clip(values, min=-most, max=most).astype(held_as)


def setup_inputs(seed: int = 0) -> dict:
    streams_of = jax.random.split(jax.random.key(seed), 13)
    context = draw_context(jax.random.fold_in(streams_of[12], 71), 0)
    latents = draw_latents(jax.random.fold_in(streams_of[12], 71), 0)
    offsets = place_ends(jax.random.randint(streams_of[2], (B,), 0, CTX_DEV * N_SEQ - LATENTS + 1), jax.random.fold_in(streams_of[2], 1), 0, CTX_DEV * N_SEQ - LATENTS).astype(jnp.int32)
    query_gain = jnp.clip(1.0 + 0.18 * jax.random.normal(streams_of[3], (D,), jnp.float32), 0.1, 1.9)
    key_gain = jnp.clip(1.0 + 0.18 * jax.random.normal(streams_of[4], (D,), jnp.float32), 0.1, 1.9)
    layer_gain = jnp.clip(1.0 + 0.18 * jax.random.normal(streams_of[5], (LAYERS, D), jnp.float32), 0.1, 1.9)
    cross_query = draw_cross_query(jax.random.fold_in(streams_of[12], 71), 0)
    cross_key = draw_cross_key(jax.random.fold_in(streams_of[12], 71), 0)
    cross_value = scatter_about(streams_of[8], (D, D), D ** -0.5, 0.1875, ((0, 32),))
    cross_out = scatter_about(streams_of[9], (D, D), D ** -0.5, 0.1875, ((0, 32),))
    layer_qkv = draw_layer_qkv(jax.random.fold_in(streams_of[12], 71), 0)
    layer_out = scatter_about(streams_of[11], (LAYERS, D, D), D ** -0.5, 0.1875, ((1, 32),))
    return dict(context=context, latents=latents, offsets=offsets, query_gain=query_gain, key_gain=key_gain, layer_gain=layer_gain, cross_query=cross_query, cross_key=cross_key, cross_value=cross_value, cross_out=cross_out, layer_qkv=layer_qkv, layer_out=layer_out)


EPSILON = 1e-06

def rms_norm(value_matrix, gain):
    value_matrix = value_matrix.astype(jnp.float32)
    scale = lax.rsqrt(lax.optimization_barrier(jnp.mean(value_matrix * value_matrix, axis=-1, keepdims=True)) + EPSILON)
    return (value_matrix * scale * gain).astype(jnp.bfloat16)

def matmul_rows(left, weight):
    flat = left.reshape(-1, left.shape[-1])
    product = jnp.dot(flat, weight, preferred_element_type=jnp.float32)
    return product.reshape(left.shape[:-1] + (weight.shape[1],))

def cross_row(operands):
    query_matrix, key_matrix, value_matrix, offset = operands
    head_width = D // H
    count = query_matrix.shape[0]
    length = key_matrix.shape[0]
    query_head_rows = query_matrix.reshape(count, H, head_width).astype(jnp.float32)
    key_head_rows = key_matrix.reshape(length, H, head_width).astype(jnp.float32)
    value_head_rows = value_matrix.reshape(length, H, head_width).astype(jnp.float32)
    score_matrix = jnp.einsum('oqi,cqi->qoc', query_head_rows, key_head_rows) * head_width ** (-0.5)
    key_pos = jnp.arange(length, dtype=jnp.int32)
    query_pos = offset + jnp.arange(count, dtype=jnp.int32)
    valid = key_pos[None, None, :] <= query_pos[None, :, None]
    top = lax.optimization_barrier(jnp.max(jnp.where(valid, score_matrix, -1e+30), axis=2, keepdims=True))
    probability_rows = jnp.where(valid, jnp.exp(score_matrix - top), 0.0).astype(jnp.bfloat16)
    denom = lax.optimization_barrier(jnp.sum(probability_rows.astype(jnp.float32), axis=2))
    numerator_sum = jnp.einsum('ycv,vys->cys', probability_rows.astype(jnp.float32), value_head_rows)
    return (numerator_sum / jnp.transpose(denom)[:, :, None]).reshape(count, D).astype(jnp.bfloat16)

def self_row(qkv):
    head_width = D // H
    count = qkv.shape[0]
    grouped = qkv.reshape(count, 3, H, head_width).astype(jnp.float32)
    query_matrix = grouped[:, 0]
    key_matrix = grouped[:, 1]
    value_matrix = grouped[:, 2]
    score_matrix = jnp.einsum('oqi,cqi->qoc', query_matrix, key_matrix) * head_width ** (-0.5)
    positions = jnp.arange(count, dtype=jnp.int32)
    valid = positions[None, None, :] <= positions[None, :, None]
    top = lax.optimization_barrier(jnp.max(jnp.where(valid, score_matrix, -1e+30), axis=2, keepdims=True))
    probability_rows = jnp.where(valid, jnp.exp(score_matrix - top), 0.0).astype(jnp.bfloat16)
    denom = lax.optimization_barrier(jnp.sum(probability_rows.astype(jnp.float32), axis=2))
    numerator_sum = jnp.einsum('ycv,vys->cys', probability_rows.astype(jnp.float32), value_matrix)
    return (numerator_sum / jnp.transpose(denom)[:, :, None]).reshape(count, D).astype(jnp.bfloat16)

def reference(context, latents, offsets, query_gain, key_gain, layer_gain, cross_query, cross_key, cross_value, cross_out, layer_qkv, layer_out):
    normed_latents = rms_norm(latents, query_gain)
    query_matrix = matmul_rows(normed_latents, cross_query).astype(jnp.bfloat16)
    normed_context = rms_norm(context, key_gain)
    key_matrix = matmul_rows(normed_context, cross_key).astype(jnp.bfloat16)
    value_matrix = matmul_rows(normed_context, cross_value).astype(jnp.bfloat16)
    attended = lax.map(cross_row, (query_matrix, key_matrix, value_matrix, offsets.astype(jnp.int32)))
    hidden = (latents.astype(jnp.float32) + matmul_rows(attended, cross_out)).astype(jnp.bfloat16)
    for layer in range(LAYERS):
        normed = rms_norm(hidden, layer_gain[layer])
        qkv = matmul_rows(normed, layer_qkv[layer]).astype(jnp.bfloat16)
        mixed = lax.map(self_row, qkv)
        hidden = (hidden.astype(jnp.float32) + matmul_rows(mixed, layer_out[layer])).astype(jnp.bfloat16)
    return hidden
```

```python
import functools

import jax
import jax.numpy as jnp
from jax import lax
from jax.experimental import pallas as pl
from jax.experimental.pallas import tpu as pltpu
from jax.sharding import PartitionSpec as P

H = 16
EPSILON = 1e-06
NEGATIVE = -1e30
AXES = ("seq", "head")
VMEM_LIMIT = 48 * 1024 * 1024
F32 = jnp.float32
BF16 = jnp.bfloat16


def rms_norm(x, gain):
    x = x.astype(F32)
    scale = lax.rsqrt(jnp.mean(x * x, axis=-1, keepdims=True) + EPSILON)
    return (x * scale * gain).astype(BF16)


def dot(a, b):
    return jnp.dot(a, b, preferred_element_type=F32)


def dot_t(a, b):
    return lax.dot_general(a, b, (((1,), (1,)), ((), ())), preferred_element_type=F32)


def head_masked(q, head, width):
    lane = lax.broadcasted_iota(jnp.int32, q.shape, 1)
    keep = (lane >= head * width) & (lane < (head + 1) * width)
    return jnp.where(keep, q, jnp.zeros_like(q))


def cross_kernel(heads, width, info, q_ref, own_ref, other_ref, out_ref):
    rows = q_ref.shape[0]
    keys = own_ref.shape[0]
    half = heads * width
    pair = 2 * width
    diff = lax.broadcasted_iota(jnp.int32, (rows, keys), 1) - lax.broadcasted_iota(jnp.int32, (rows, keys), 0)
    valid_own = diff <= info[0] - info[1]
    valid_other = diff <= info[0] - info[2]
    ones = jnp.ones((keys, pair), BF16)
    lane = lax.broadcasted_iota(jnp.int32, (rows, pair), 1)
    stat_lane = lax.broadcasted_iota(jnp.int32, (rows, 128), 1)
    stats = jnp.full((rows, 128), NEGATIVE, F32)
    for p in range(heads // 2):
        cols = slice(p * pair, (p + 1) * pair)
        vcols = slice(half + p * pair, half + (p + 1) * pair)
        q = q_ref[:, cols] * jnp.asarray(width ** -0.5, BF16)
        v_own = jnp.concatenate([own_ref[:, vcols], ones], axis=1)
        v_other = jnp.concatenate([other_ref[:, vcols], ones], axis=1)
        outs = []
        for e in range(2):
            qm = head_masked(q, e, width)
            s0 = jnp.where(valid_own, dot_t(qm, own_ref[:, cols]), NEGATIVE)
            s1 = jnp.where(valid_other, dot_t(qm, other_ref[:, cols]), NEGATIVE)
            top = jnp.maximum(jnp.max(s0, axis=1, keepdims=True), jnp.max(s1, axis=1, keepdims=True))
            p0 = jnp.exp(s0 - top).astype(BF16)
            p1 = jnp.exp(s1 - top).astype(BF16)
            o = dot(p0, v_own) + dot(p1, v_other)
            total = o[:, pair:]
            outs.append(o[:, :pair] / total)
            lse = jnp.where(top > 0.1 * NEGATIVE, top + jnp.log(total[:, :1]), NEGATIVE)
            stats = jnp.where(stat_lane == 2 * p + e, lse, stats)
        out_ref[:rows, cols] = jnp.where(lane < width, outs[0], outs[1]).astype(BF16)
    st = jnp.transpose(stats)[:heads]
    hi = st.astype(BF16)
    rest = st - hi.astype(F32)
    mid = rest.astype(BF16)
    low = (rest - mid.astype(F32)).astype(BF16)
    pad = half - 2 * rows
    top_part = [hi, mid] + ([jnp.zeros((heads, pad), BF16)] if pad else [])
    low_part = [low, jnp.zeros((heads, half - rows), BF16)]
    tail = jnp.concatenate([jnp.concatenate(top_part, axis=1), jnp.concatenate(low_part, axis=1)], axis=0)
    out_ref[rows:, :] = tail


def combine_kernel(heads, width, info, *refs):
    parts, (keep_ref, send_ref) = refs[:-2], refs[-2:]
    rows = keep_ref.shape[0] * 2
    half = heads * width
    lses = []
    for part in parts:
        hi = part[rows : rows + heads, :rows].astype(F32)
        mid = part[rows : rows + heads, rows : 2 * rows].astype(F32)
        low = part[rows + heads : rows + 2 * heads, :rows].astype(F32)
        lses.append(hi + mid + low)
    top = functools.reduce(jnp.maximum, lses)
    weights = [jnp.exp(lse - top) for lse in lses]
    total = functools.reduce(jnp.add, weights)
    spread = (
        lax.broadcasted_iota(jnp.int32, (heads, half), 1) // width
        == lax.broadcasted_iota(jnp.int32, (heads, half), 0)
    ).astype(F32)
    acc = jnp.zeros((rows, half), F32)
    for part, weight in zip(parts, weights):
        wide = lax.dot_general(
            weight / total, spread, (((0,), (0,)), ((), ())), precision=lax.Precision.HIGHEST, preferred_element_type=F32
        )
        acc = acc + wide * part[:rows, :].astype(F32)
    acc = acc.astype(BF16)
    odd = info[0] == 1
    first, second = acc[: rows // 2], acc[rows // 2 :]
    keep_ref[...] = jnp.where(odd, second, first)
    send_ref[...] = jnp.where(odd, first, second)


def cross_out_kernel(info, keep_ref, got_ref, lat_ref, w_ref, out_ref):
    x = info[0]
    update = dot(keep_ref[...], w_ref[x]) + dot(got_ref[...], w_ref[1 - x])
    out_ref[...] = (lat_ref[...].astype(F32) + update).astype(BF16)


def self_attention(qkv, mixed_ref, count, cols, width):
    step = min(count, 256)
    diff = lax.broadcasted_iota(jnp.int32, (step, step), 1) - lax.broadcasted_iota(jnp.int32, (step, step), 0)
    causal = diff <= 0
    heads = cols // width
    lane = lax.broadcasted_iota(jnp.int32, (step, cols), 1)
    for i in range(count // step):
        here = slice(i * step, (i + 1) * step)
        before = slice(0, i * step)
        q = qkv[here, :cols] * jnp.asarray(width ** -0.5, BF16)
        out = None
        for e in range(heads):
            qm = head_masked(q, e, width)
            s1 = jnp.where(causal, dot_t(qm, qkv[here, cols : 2 * cols]), NEGATIVE)
            top = jnp.max(s1, axis=1, keepdims=True)
            if i:
                s0 = dot_t(qm, qkv[before, cols : 2 * cols])
                top = jnp.maximum(top, jnp.max(s0, axis=1, keepdims=True))
            p1 = jnp.exp(s1 - top).astype(BF16)
            o = dot(p1, jnp.concatenate([qkv[here, 2 * cols :], jnp.ones((step, 128), BF16)], axis=1))
            if i:
                p0 = jnp.exp(s0 - top).astype(BF16)
                o = o + dot(p0, jnp.concatenate([qkv[before, 2 * cols :], jnp.ones((i * step, 128), BF16)], axis=1))
            o = o[:, :cols] / o[:, cols : cols + 1]
            out = o if out is None else jnp.where(lane < e * width, out, o)
        mixed_ref[here, :] = out.astype(BF16)


def first_layer_kernel(width, info, *refs):
    *blocks, w_ref, gain_ref, hidden_ref, mixed_ref, qkv = refs
    rows = blocks[0].shape[0]
    gain = gain_ref[...]
    for j, block in enumerate(blocks):
        at = pl.multiple_of((info[0] ^ j) * rows, rows)
        x = block[...]
        hidden_ref[pl.ds(at, rows), :] = x
        qkv[pl.ds(at, rows), :] = dot(rms_norm(x, gain), w_ref[...]).astype(BF16)
    self_attention(qkv, mixed_ref, rows * len(blocks), w_ref.shape[1] // 3, width)


def next_layer_kernel(width, info, *refs):
    *blocks, out_w_ref, hidden_ref, w_ref, gain_ref, own_ref, mixed_ref, qkv, hidden_new = refs
    count = hidden_ref.shape[0]
    gain = gain_ref[...]
    step = min(count, 256)
    for i in range(count // step):
        here = slice(i * step, (i + 1) * step)
        update = hidden_ref[here, :].astype(F32)
        for j, block in enumerate(blocks):
            update = update + dot(block[here, :], out_w_ref[info[0] ^ j])
        x = update.astype(BF16)
        hidden_new[here, :] = x
        qkv[here, :] = dot(rms_norm(x, gain), w_ref[...]).astype(BF16)
    rows = own_ref.shape[0]
    own_ref[...] = hidden_new[pl.ds(pl.multiple_of(info[0] * rows, rows), rows), :]
    self_attention(qkv, mixed_ref, count, w_ref.shape[1] // 3, width)


def last_kernel(info, *refs):
    *blocks, out_w_ref, hidden_ref, out_ref = refs
    update = hidden_ref[...].astype(F32)
    for j, block in enumerate(blocks):
        update = update + dot(block[...], out_w_ref[info[0] ^ j])
    out_ref[...] = update.astype(BF16)


def call(kernel, name, info, operands, outs, scratch=()):
    vmem = pl.BlockSpec(memory_space=pltpu.VMEM)
    return pl.pallas_call(
        kernel,
        name=name,
        out_shape=outs,
        in_specs=[pl.BlockSpec(memory_space=pltpu.SMEM)] + [vmem] * len(operands),
        out_specs=jax.tree.map(lambda _: vmem, outs),
        scratch_shapes=list(scratch),
        compiler_params=pltpu.CompilerParams(vmem_limit_bytes=VMEM_LIMIT),
    )(info, *operands)


def per_device(
    context,
    latents,
    offsets,
    query_gain,
    key_gain,
    layer_gain,
    cross_query,
    cross_key,
    cross_value,
    cross_out,
    layer_qkv,
    layer_out,
):
    ns, nh = lax.axis_size("seq"), lax.axis_size("head")
    s, h = lax.axis_index("seq"), lax.axis_index("head")
    context, latents = context[0], latents[0]
    ctx_len, width_all = context.shape
    count = latents.shape[0]
    layers = layer_qkv.shape[0]
    head_width = width_all // H
    half = width_all // 2
    block = cross_query.shape[0]
    members = ns
    rows = count // members
    cols = width_all // members
    us = ns // 2
    s_bits = [1 << b for b in reversed(range(ns.bit_length() - 1))]
    h_bits = [1 << b for b in reversed(range(nh.bit_length() - 1))]
    x = s & 1
    t = s // us
    u = s % us
    c = h & 1
    v = h // 2
    g = c * us + u
    shape = jax.ShapeDtypeStruct

    def move(array, to):
        pairs = [(i * nh + j, (lambda d: d[0] * nh + d[1])(to(i, j))) for i in range(ns) for j in range(nh)]
        return lax.ppermute(array, AXES, pairs)

    def flip(array, ds, dh):
        return move(array, lambda i, j: (i ^ ds, j ^ dh))

    axis_of = {("s", b): k for k, b in enumerate(s_bits)} | {("h", b): len(s_bits) + k for k, b in enumerate(h_bits)}
    blank = (1,) * len(axis_of)

    def ordered(mine, other, kind, bit, lead):
        axis = lead + axis_of[(kind, bit)]
        high = ((s if kind == "s" else h) & bit) != 0
        return jnp.where(
            high, jnp.concatenate([other, mine], axis=axis), jnp.concatenate([mine, other], axis=axis)
        )

    def gather(array, order, lead=0):
        for kind, bit in order:
            other = flip(array, bit if kind == "s" else 0, bit if kind == "h" else 0)
            array = ordered(array, other, kind, bit, lead)
        return array

    def trade(array, kind, bit, lead=0):
        mine_at = (((s if kind == "s" else h) & bit) != 0).astype(jnp.int32)
        keep = lax.dynamic_index_in_dim(array, mine_at, 0, keepdims=False)
        send = lax.dynamic_index_in_dim(array, 1 - mine_at, 0, keepdims=False)
        other = flip(send, bit if kind == "s" else 0, bit if kind == "h" else 0)
        return ordered(keep, other, kind, bit, lead)

    z_order = [("s", b) for b in s_bits if b != 1]
    y_order = [("h", b) for b in h_bits if b != 1]
    x_bit, c_bit = ("s", 1), ("h", 1)

    def halves(weights):
        return jnp.stack(
            [jnp.concatenate([w[:, k * half : (k + 1) * half] for w in weights], axis=1) for k in range(2)]
        ).reshape((2,) + blank + (block, half * len(weights)))

    context_other = None
    kv_w = trade(halves([cross_key, cross_value]), *x_bit)
    q_w = trade(halves([cross_query]), *x_bit)
    context_other = flip(context, 1, 0)
    kv_w = gather(kv_w, z_order + y_order + [c_bit]).reshape(width_all, 2 * half)
    q_w = gather(q_w, y_order + z_order + [c_bit]).reshape(width_all, half)
    out_w = gather(cross_out.reshape(blank + (block, width_all)), z_order + y_order + [x_bit, c_bit])
    out_w = out_w.reshape(2, half, width_all)

    qkv_w = layer_qkv.reshape(layers, block, 3, 2, us // 2, 2, cols)
    qkv_w = jnp.transpose(qkv_w, (5, 4, 3, 0, 1, 2, 6)).reshape((2, us // 2, 2, layers) + blank + (block, 3 * cols))
    lead = 4
    keep_lead = 3
    qkv_w = trade(qkv_w, *x_bit, lead=keep_lead)
    for b in [b for b in s_bits if b not in (1, us)]:
        rest = qkv_w.shape[0] // 2
        qkv_w = qkv_w.reshape((2, rest) + qkv_w.shape[1:])
        qkv_w = trade(qkv_w, "s", b, lead=3)
    qkv_w = qkv_w.reshape(qkv_w.shape[1:])
    qkv_w = trade(qkv_w, *c_bit, lead=1)
    qkv_w = gather(qkv_w, [("s", us)] + y_order, lead=1).reshape(layers, width_all, 3 * cols)
    last_w = gather(
        layer_out.reshape((layers,) + blank + (block, width_all)), z_order + [x_bit] + y_order + [c_bit], lead=1
    ).reshape(layers, members, cols, width_all)

    kv_own = dot(rms_norm(context, key_gain), kv_w).astype(BF16)
    kv_other = dot(rms_norm(context_other, key_gain), kv_w).astype(BF16)
    queries = dot(rms_norm(latents, query_gain), q_w).astype(BF16)

    dests = ns // 2
    span = count // dests
    z_low = u // 2
    heads = H // 2
    received = []
    for b in range(2):
        for a in range(us // 2):
            at = ((t ^ b) * (us // 2) + (z_low ^ a)) * span
            q = lax.dynamic_slice_in_dim(queries, at, span, 0)
            info = jnp.stack([offsets[0] + at, s * ctx_len, (s ^ 1) * ctx_len]).astype(jnp.int32)
            part = call(
                functools.partial(cross_kernel, heads, head_width),
                "cross",
                info,
                (q, kv_own, kv_other),
                shape((span + 2 * heads, half), BF16),
            )

            def to(i, j, a=a, b=b):
                ti, ui = i // us, i % us
                return ((j & 1) * us + (ui ^ (2 * a)), (j & ~1) | (ti ^ b))

            received.append(move(part, to))
    x_info = x.astype(jnp.int32).reshape(1)
    keep, send = call(
        functools.partial(combine_kernel, heads, head_width),
        "combine",
        x_info,
        tuple(received),
        (shape((rows, half), BF16), shape((rows, half), BF16)),
    )
    got = flip(send, 1, 0)

    lat_mine = lax.dynamic_slice_in_dim(latents, g * rows, rows, 0)
    lat_send = lax.dynamic_slice_in_dim(latents, ((1 - c) * us + u) * rows, rows, 0)
    lat_rows = jnp.where(c == t, lat_mine, flip(lat_send, 0, 1))
    hidden = call(cross_out_kernel, "cross_out", x_info, (keep, got, lat_rows, out_w), shape((rows, width_all), BF16))

    def group_gather(array):
        near = [array] + [flip(array, k, 0) for k in range(1, us)]
        return near + [flip(n, 0, 1) for n in near]

    g_info = g.astype(jnp.int32).reshape(1)
    gains = layer_gain.reshape(layers, 1, width_all)
    qkv_scratch = pltpu.VMEM((count, 3 * cols), BF16)
    hidden, mixed = call(
        functools.partial(first_layer_kernel, head_width),
        "layer_first",
        g_info,
        (*group_gather(hidden), qkv_w[0], gains[0]),
        (shape((count, width_all), BF16), shape((count, cols), BF16)),
        [qkv_scratch],
    )
    own = None
    for layer in range(1, layers):
        own, mixed = call(
            functools.partial(next_layer_kernel, head_width),
            "layer_next",
            g_info,
            (*group_gather(mixed), last_w[layer - 1], hidden, qkv_w[layer], gains[layer]),
            (shape((rows, width_all), BF16), shape((count, cols), BF16)),
            [qkv_scratch, pltpu.VMEM((count, width_all), BF16)],
        )

    own = move(own, lambda i, j: ((j & 1) * us + i % us, (j & ~1) | (i // us)))
    pieces = []
    for b in range(2):
        for a in range(us):
            piece = lax.dynamic_slice_in_dim(mixed, ((c ^ b) * us + (u ^ a)) * rows, rows, 0)

            def home(i, j, a=a, b=b):
                return (((j & 1) ^ b) * us + ((i % us) ^ a), (j & ~1) | (i // us))

            pieces.append(move(piece, home))
    out = call(
        last_kernel,
        "last",
        s.astype(jnp.int32).reshape(1),
        (*pieces, last_w[layers - 1], own),
        shape((rows, width_all), BF16),
    )
    return out[None]


def solution(mesh):
    return jax.shard_map(
        per_device,
        mesh=mesh,
        in_specs=(
            P("head", "seq", None),
            P("head", None, None),
            P("head"),
            P(),
            P(),
            P(),
            P(("seq", "head"), None),
            P(("seq", "head"), None),
            P(("seq", "head"), None),
            P(("seq", "head"), None),
            P(None, ("seq", "head"), None),
            P(None, ("seq", "head"), None),
        ),
        out_specs=P("head", "seq", None),
        check_vma=False,
    )
```

```python
import functools

import jax
import jax.numpy as jnp
from jax import lax
from jax.experimental import pallas as pl
from jax.experimental.pallas import tpu as pltpu
from jax.sharding import PartitionSpec as P

H = 16
EPSILON = 1e-06
NEGATIVE = -1e30
AXES = ("seq", "head")
VMEM_LIMIT = 48 * 1024 * 1024
F32 = jnp.float32
BF16 = jnp.bfloat16


def rms_norm(x, gain):
    x = x.astype(F32)
    scale = lax.rsqrt(jnp.mean(x * x, axis=-1, keepdims=True) + EPSILON)
    return (x * scale * gain).astype(BF16)


def dot(a, b):
    return jnp.dot(a, b, preferred_element_type=F32)


def dot_t(a, b):
    return lax.dot_general(a, b, (((1,), (1,)), ((), ())), preferred_element_type=F32)


def head_masked(q, head, width):
    lane = lax.broadcasted_iota(jnp.int32, q.shape, 1)
    keep = (lane >= head * width) & (lane < (head + 1) * width)
    return jnp.where(keep, q, jnp.zeros_like(q))


def assemble(odd, mine_ref, other_ref, out_ref, block):
    def body(k, carry):
        here = pl.ds(pl.multiple_of(k * block, block), block)
        out_ref[pl.ds(pl.multiple_of((2 * k + odd) * block, block), block), :] = mine_ref[here, :]
        out_ref[pl.ds(pl.multiple_of((2 * k + 1 - odd) * block, block), block), :] = other_ref[here, :]
        return carry

    lax.fori_loop(0, mine_ref.shape[0] // block, body, 0)


def each(count, step, body):
    def one(i, carry):
        body(pl.ds(pl.multiple_of(i * step, step), step))
        return carry

    lax.fori_loop(0, count // step, one, 0)


def project_kernel(block, info, *refs):
    own, other, lat, kg, qg, a0, a1, b0, b1, kv_own, kv_other, q_ref, a, b = refs
    half = kv_own.shape[1] // 2
    part = a.shape[1] - half
    assemble(info[0], a0, a1, a, block)
    assemble(info[0], b0, b1, b, block)
    step = min(256, own.shape[0])
    for src, dst in ((own, kv_own), (other, kv_other)):

        def context_rows(here, src=src, dst=dst):
            n = rms_norm(src[here, :], kg[...])
            dst[here, :half] = dot(n, a[:, :half]).astype(BF16)
            dst[here, half:] = dot(n, b[:, :half]).astype(BF16)

        each(src.shape[0], step, context_rows)

    def latent_rows(here):
        n = rms_norm(lat[here, :], qg[...])
        q_ref[here, :part] = dot(n, a[:, half:]).astype(BF16)
        q_ref[here, part:] = dot(n, b[:, half:]).astype(BF16)

    each(lat.shape[0], step, latent_rows)


def cross_kernel(heads, width, info, q_ref, own_ref, other_ref, out_ref):
    rows = q_ref.shape[0]
    keys = own_ref.shape[0]
    half = heads * width
    pair = 2 * width
    diff = lax.broadcasted_iota(jnp.int32, (rows, keys), 1) - lax.broadcasted_iota(jnp.int32, (rows, keys), 0)
    valid_own = diff <= info[0] - info[1]
    valid_other = diff <= info[0] - info[2]
    ones = jnp.ones((keys, pair), BF16)
    lane = lax.broadcasted_iota(jnp.int32, (rows, pair), 1)
    stat_lane = lax.broadcasted_iota(jnp.int32, (rows, 128), 1)

    def one_pair(p, stats):
        cols = pl.ds(pl.multiple_of(p * pair, pair), pair)
        vcols = pl.ds(pl.multiple_of(half + p * pair, pair), pair)
        q = q_ref[:, cols] * jnp.asarray(width ** -0.5, BF16)
        v_own = jnp.concatenate([own_ref[:, vcols], ones], axis=1)
        v_other = jnp.concatenate([other_ref[:, vcols], ones], axis=1)
        outs = []
        for e in range(2):
            qm = head_masked(q, e, width)
            s0 = jnp.where(valid_own, dot_t(qm, own_ref[:, cols]), NEGATIVE)
            s1 = jnp.where(valid_other, dot_t(qm, other_ref[:, cols]), NEGATIVE)
            top = jnp.maximum(jnp.max(s0, axis=1, keepdims=True), jnp.max(s1, axis=1, keepdims=True))
            p0 = jnp.exp(s0 - top).astype(BF16)
            p1 = jnp.exp(s1 - top).astype(BF16)
            o = dot(p0, v_own) + dot(p1, v_other)
            total = o[:, pair:]
            outs.append(o[:, :pair] / total)
            lse = jnp.where(top > 0.1 * NEGATIVE, top + jnp.log(total[:, :1]), NEGATIVE)
            stats = jnp.where(stat_lane == 2 * p + e, lse, stats)
        out_ref[:rows, cols] = jnp.where(lane < width, outs[0], outs[1]).astype(BF16)
        return stats

    stats = lax.fori_loop(0, heads // 2, one_pair, jnp.full((rows, 128), NEGATIVE, F32), unroll=True)
    st = jnp.transpose(stats)[:heads]
    hi = st.astype(BF16)
    rest = st - hi.astype(F32)
    mid = rest.astype(BF16)
    low = (rest - mid.astype(F32)).astype(BF16)
    pad = half - 2 * rows
    top_part = [hi, mid] + ([jnp.zeros((heads, pad), BF16)] if pad else [])
    low_part = [low, jnp.zeros((heads, half - rows), BF16)]
    tail = jnp.concatenate([jnp.concatenate(top_part, axis=1), jnp.concatenate(low_part, axis=1)], axis=0)
    out_ref[rows:, :] = tail


def combine_kernel(heads, width, info, *refs):
    parts, (keep_ref, send_ref) = refs[:-2], refs[-2:]
    rows = keep_ref.shape[0] * 2
    half = heads * width
    lses = []
    for part in parts:
        hi = part[rows : rows + heads, :rows].astype(F32)
        mid = part[rows : rows + heads, rows : 2 * rows].astype(F32)
        low = part[rows + heads : rows + 2 * heads, :rows].astype(F32)
        lses.append(hi + mid + low)
    top = functools.reduce(jnp.maximum, lses)
    weights = [jnp.exp(lse - top) for lse in lses]
    total = functools.reduce(jnp.add, weights)
    spread = (
        lax.broadcasted_iota(jnp.int32, (heads, half), 1) // width
        == lax.broadcasted_iota(jnp.int32, (heads, half), 0)
    ).astype(F32)
    acc = jnp.zeros((rows, half), F32)
    for part, weight in zip(parts, weights):
        wide = lax.dot_general(
            weight / total, spread, (((0,), (0,)), ((), ())), precision=lax.Precision.HIGHEST, preferred_element_type=F32
        )
        acc = acc + wide * part[:rows, :].astype(F32)
    acc = acc.astype(BF16)
    odd = info[0] == 1
    first, second = acc[: rows // 2], acc[rows // 2 :]
    keep_ref[...] = jnp.where(odd, second, first)
    send_ref[...] = jnp.where(odd, first, second)


def fetch(stored, held, sem):
    copies = [
        pltpu.make_async_copy(ref.at[index], to, sem.at[k]) for k, ((ref, index), to) in enumerate(zip(stored, held))
    ]
    for copy in copies:
        copy.start()
    return copies


def cross_out_kernel(info, keep_ref, got_ref, lat_ref, full_ref, out_ref, w_ref, sem):
    (copy,) = fetch([(full_ref, 0)], [w_ref], sem)
    copy.wait()
    x = info[0]
    half = keep_ref.shape[1]
    mine = w_ref[pl.ds(pl.multiple_of(x * half, half), half), :]
    theirs = w_ref[pl.ds(pl.multiple_of((1 - x) * half, half), half), :]
    update = dot(keep_ref[...], mine) + dot(got_ref[...], theirs)
    out_ref[...] = (lat_ref[...].astype(F32) + update).astype(BF16)


def self_attention(qkv, mixed_ref, count, cols, width):
    step = min(count, 256)
    diff = lax.broadcasted_iota(jnp.int32, (step, step), 1) - lax.broadcasted_iota(jnp.int32, (step, step), 0)
    causal = diff <= 0
    heads = cols // width
    lane = lax.broadcasted_iota(jnp.int32, (step, cols), 1)
    for i in range(count // step):
        here = slice(i * step, (i + 1) * step)
        before = slice(0, i * step)
        q = qkv[here, :cols] * jnp.asarray(width ** -0.5, BF16)
        v1 = jnp.concatenate([qkv[here, 2 * cols :], jnp.ones((step, 128), BF16)], axis=1)
        if i:
            v0 = jnp.concatenate([qkv[before, 2 * cols :], jnp.ones((i * step, 128), BF16)], axis=1)

        def one_head(e, out):
            qm = head_masked(q, e, width)
            s1 = jnp.where(causal, dot_t(qm, qkv[here, cols : 2 * cols]), NEGATIVE)
            top = jnp.max(s1, axis=1, keepdims=True)
            if i:
                s0 = dot_t(qm, qkv[before, cols : 2 * cols])
                top = jnp.maximum(top, jnp.max(s0, axis=1, keepdims=True))
            p1 = jnp.exp(s1 - top).astype(BF16)
            o = dot(p1, v1)
            if i:
                o = o + dot(jnp.exp(s0 - top).astype(BF16), v0)
            o = o[:, :cols] / o[:, cols : cols + 1]
            return jnp.where(lane < e * width, out, o)

        out = lax.fori_loop(0, heads, one_head, jnp.zeros((step, cols), F32), unroll=True)
        mixed_ref[here, :] = out.astype(BF16)


def first_layer_kernel(width, info, *refs):
    *blocks, layers_ref, gain_ref, hidden_ref, mixed_ref, qkv, w_ref, sem = refs
    (copy,) = fetch([(layers_ref, 0)], [w_ref], sem)
    copy.wait()
    rows = blocks[0].shape[0]
    gain = gain_ref[...]
    for j, block in enumerate(blocks):
        at = pl.multiple_of((info[0] ^ j) * rows, rows)
        x = block[...]
        hidden_ref[pl.ds(at, rows), :] = x
        qkv[pl.ds(at, rows), :] = dot(rms_norm(x, gain), w_ref[...]).astype(BF16)
    self_attention(qkv, mixed_ref, rows * len(blocks), w_ref.shape[1] // 3, width)


def next_layer_kernel(width, layer, info, *refs):
    *blocks, full_ref, hidden_ref, layers_ref, gain_ref, own_ref, mixed_ref = refs[:-6]
    qkv, hidden_new, joined, out_w_ref, w_ref, sem = refs[-6:]
    copies = fetch([(full_ref, layer), (layers_ref, layer)], [out_w_ref, w_ref], sem)
    for copy in copies:
        copy.wait()
    count = hidden_ref.shape[0]
    cols = blocks[0].shape[1]
    gain = gain_ref[...]
    step = min(count, 256)
    wide = cols % 128 == 0

    def rows_of(here):
        update = hidden_ref[here, :].astype(F32)
        if wide:
            for j, block in enumerate(blocks):
                joined[:, pl.ds(pl.multiple_of((info[0] ^ j) * cols, cols), cols)] = block[here, :]
            update = update + dot(joined[...], out_w_ref[...])
        else:
            for j, block in enumerate(blocks):
                at = pl.multiple_of((info[0] ^ j) * cols, cols)
                update = update + dot(block[here, :], out_w_ref[pl.ds(at, cols), :])
        x = update.astype(BF16)
        hidden_new[here, :] = x
        qkv[here, :] = dot(rms_norm(x, gain), w_ref[...]).astype(BF16)

    each(count, step, rows_of)
    rows = own_ref.shape[0]
    own_ref[...] = hidden_new[pl.ds(pl.multiple_of(info[0] * rows, rows), rows), :]
    self_attention(qkv, mixed_ref, count, w_ref.shape[1] // 3, width)


def last_kernel(layer, info, *refs):
    *blocks, full_ref, hidden_ref, out_ref, w_ref, sem = refs
    (copy,) = fetch([(full_ref, layer)], [w_ref], sem)
    copy.wait()
    update = hidden_ref[...].astype(F32)
    cols = blocks[0].shape[2]
    for a, block in enumerate(blocks):
        for e in range(2):
            at = pl.multiple_of((e * len(blocks) + (info[0] ^ a)) * cols, cols)
            update = update + dot(block[e], w_ref[pl.ds(at, cols), :])
    out_ref[...] = update.astype(BF16)


def call(kernel, name, info, operands, outs, scratch=()):
    vmem = pl.BlockSpec(memory_space=pltpu.VMEM)

    def spec(operand):
        return pl.BlockSpec(memory_space=pl.ANY) if isinstance(operand, tuple) else vmem

    in_specs = [pl.BlockSpec(memory_space=pltpu.SMEM)] + [spec(o) for o in operands]
    stored = [o[0] for o in operands if isinstance(o, tuple)]
    scratch = list(scratch) + [pltpu.VMEM(o.shape[1:], o.dtype) for o in stored]
    scratch += [pltpu.SemaphoreType.DMA((len(stored),))] if stored else []
    operands = [o[0] if isinstance(o, tuple) else o for o in operands]
    return pl.pallas_call(
        kernel,
        name=name,
        out_shape=outs,
        in_specs=in_specs,
        out_specs=jax.tree.map(lambda _: vmem, outs),
        scratch_shapes=list(scratch),
        compiler_params=pltpu.CompilerParams(vmem_limit_bytes=VMEM_LIMIT),
    )(info, *operands)


def per_device(
    context,
    latents,
    offsets,
    query_gain,
    key_gain,
    layer_gain,
    cross_query,
    cross_key,
    cross_value,
    cross_out,
    layer_qkv,
    layer_out,
):
    ns, nh = lax.axis_size("seq"), lax.axis_size("head")
    s, h = lax.axis_index("seq"), lax.axis_index("head")
    context, latents = context[0], latents[0]
    ctx_len, width_all = context.shape
    count = latents.shape[0]
    layers = layer_qkv.shape[0]
    head_width = width_all // H
    half = width_all // 2
    block = cross_query.shape[0]
    members = ns
    rows = count // members
    cols = width_all // members
    us = ns // 2
    s_bits = [1 << b for b in reversed(range(ns.bit_length() - 1))]
    h_bits = [1 << b for b in reversed(range(nh.bit_length() - 1))]
    x = s & 1
    t = s // us
    u = s % us
    c = h & 1
    v = h // 2
    g = c * us + u
    shape = jax.ShapeDtypeStruct

    def move(array, to):
        pairs = [(i * nh + j, (lambda d: d[0] * nh + d[1])(to(i, j))) for i in range(ns) for j in range(nh)]
        return lax.ppermute(array, AXES, pairs)

    def flip(array, ds, dh):
        return move(array, lambda i, j: (i ^ ds, j ^ dh))

    axis_of = {("s", b): k for k, b in enumerate(s_bits)} | {("h", b): len(s_bits) + k for k, b in enumerate(h_bits)}
    blank = (1,) * len(axis_of)

    def ordered(mine, other, kind, bit, lead):
        axis = lead + axis_of[(kind, bit)]
        high = ((s if kind == "s" else h) & bit) != 0
        return jnp.where(
            high, jnp.concatenate([other, mine], axis=axis), jnp.concatenate([mine, other], axis=axis)
        )

    def gather(array, order, lead=0):
        for kind, bit in order:
            other = flip(array, bit if kind == "s" else 0, bit if kind == "h" else 0)
            array = ordered(array, other, kind, bit, lead)
        return array

    def trade(array, kind, bit, lead=0):
        mine_at = (((s if kind == "s" else h) & bit) != 0).astype(jnp.int32)
        keep = lax.dynamic_index_in_dim(array, mine_at, 0, keepdims=False)
        send = lax.dynamic_index_in_dim(array, 1 - mine_at, 0, keepdims=False)
        other = flip(send, bit if kind == "s" else 0, bit if kind == "h" else 0)
        return ordered(keep, other, kind, bit, lead)

    z_order = [("s", b) for b in s_bits if b != 1]
    y_order = [("h", b) for b in h_bits if b != 1]
    x_bit, c_bit = ("s", 1), ("h", 1)

    def last_pair(array, lead=0):
        other = flip(array, 0, 1)
        flat = array.shape[:lead] + (-1, array.shape[-1])
        return array.reshape(flat), other.reshape(flat)

    def halves(big, small, k):
        quarter = half // 2
        return jnp.stack(
            [
                jnp.concatenate(
                    [big[:, x * half : (x + 1) * half], small[:, x * half + k * quarter : x * half + (k + 1) * quarter]],
                    axis=1,
                )
                for x in range(2)
            ]
        ).reshape((2,) + blank + (block, half + quarter))

    def tie(array, *others):
        others = [o for o in others if o is not None]
        return lax.optimization_barrier((array, *others))[0] if others else array

    full = lax.all_gather(jnp.concatenate([cross_out[None], layer_out]), AXES, axis=1, tiled=True)
    a_w = trade(halves(cross_key, cross_query, 0), *x_bit)
    b_w = trade(halves(cross_value, cross_query, 1), *x_bit)
    qkv_w = layer_qkv.reshape(layers, block, 3, 2, us // 2, 2, cols)
    qkv_w = jnp.transpose(qkv_w, (5, 4, 3, 0, 1, 2, 6)).reshape((2, us // 2, 2, layers) + blank + (block, 3 * cols))
    qkv_w = trade(tie(qkv_w, a_w, b_w), *x_bit, lead=3)
    context_other = flip(tie(context, qkv_w), 1, 0)
    a_w = gather(a_w, z_order)
    b_w = gather(b_w, y_order)
    for b in [b for b in s_bits if b not in (1, us)]:
        qkv_w = tie(qkv_w, a_w, b_w).reshape((2, qkv_w.shape[0] // 2) + qkv_w.shape[1:])
        qkv_w = trade(qkv_w, "s", b, lead=3)
    qkv_w = trade(qkv_w.reshape(qkv_w.shape[1:]), *c_bit, lead=1)
    a_w = gather(a_w, y_order)
    b_w = gather(b_w, z_order)
    a_pair = last_pair(a_w)
    b_pair = last_pair(b_w)
    qkv_w = gather(tie(qkv_w, a_pair[1], b_pair[1]), [("s", us)], lead=1)

    c_info = c.astype(jnp.int32).reshape(1)
    kv_shape = shape((ctx_len, 2 * half), BF16)
    w_scratch = pltpu.VMEM((width_all, half + half // 2), BF16)
    kv_own, kv_other, queries = call(
        functools.partial(project_kernel, block),
        "project",
        c_info,
        (context, context_other, latents, key_gain.reshape(1, -1), query_gain.reshape(1, -1), *a_pair, *b_pair),
        (kv_shape, kv_shape, shape((count, half), BF16)),
        [w_scratch, w_scratch],
    )

    dests = ns // 2
    span = count // dests
    z_low = u // 2
    heads = H // 2
    received = []
    for b in range(2):
        for a in range(us // 2):
            at = ((t ^ b) * (us // 2) + (z_low ^ a)) * span
            q = lax.dynamic_slice_in_dim(queries, at, span, 0)
            info = jnp.stack([offsets[0] + at, s * ctx_len, (s ^ 1) * ctx_len]).astype(jnp.int32)
            part = call(
                functools.partial(cross_kernel, heads, head_width),
                "cross",
                info,
                (q, kv_own, kv_other),
                shape((span + 2 * heads, half), BF16),
            )

            def to(i, j, a=a, b=b):
                ti, ui = i // us, i % us
                return ((j & 1) * us + (ui ^ (2 * a)), (j & ~1) | (ti ^ b))

            received.append(move(part, to))
            if len(received) == 2:
                qkv_w = gather(tie(qkv_w, part), y_order, lead=1).reshape(layers, width_all, 3 * cols)
    x_info = x.astype(jnp.int32).reshape(1)
    keep, send = call(
        functools.partial(combine_kernel, heads, head_width),
        "combine",
        x_info,
        tuple(received),
        (shape((rows, half), BF16), shape((rows, half), BF16)),
    )
    got = flip(send, 1, 0)

    lat_mine = lax.dynamic_slice_in_dim(latents, g * rows, rows, 0)
    lat_send = lax.dynamic_slice_in_dim(latents, ((1 - c) * us + u) * rows, rows, 0)
    lat_rows = jnp.where(c == t, lat_mine, flip(lat_send, 0, 1))
    hidden = call(
        cross_out_kernel,
        "cross_out",
        x_info,
        (keep, got, lat_rows, (full, 0)),
        shape((rows, width_all), BF16),
    )

    def group_gather(array):
        near = [array] + [flip(array, k, 0) for k in range(1, us)]
        return near + [flip(n, 0, 1) for n in near]

    g_info = g.astype(jnp.int32).reshape(1)
    gains = layer_gain.reshape(layers, 1, width_all)
    qkv_scratch = pltpu.VMEM((count, 3 * cols), BF16)
    hidden, mixed = call(
        functools.partial(first_layer_kernel, head_width),
        "layer_first",
        g_info,
        (*group_gather(hidden), (qkv_w, 0), gains[0]),
        (shape((count, width_all), BF16), shape((count, cols), BF16)),
        [qkv_scratch],
    )
    own = None
    for layer in range(1, layers):
        own, mixed = call(
            functools.partial(next_layer_kernel, head_width, layer),
            "layer_next",
            g_info,
            (*group_gather(mixed), (full, layer), hidden, (qkv_w, layer), gains[layer]),
            (shape((rows, width_all), BF16), shape((count, cols), BF16)),
            [qkv_scratch, pltpu.VMEM((count, width_all), BF16), pltpu.VMEM((min(count, 256), width_all), BF16)],
        )

    own = move(own, lambda i, j: ((j & 1) * us + i % us, (j & ~1) | (i // us)))
    split = mixed.reshape(2, us, rows, cols)
    keep = lax.dynamic_index_in_dim(split, c, 0, keepdims=False)
    other = flip(lax.dynamic_index_in_dim(split, 1 - c, 0, keepdims=False), 0, 1)
    both = jnp.where(c == 1, jnp.stack([other, keep]), jnp.stack([keep, other]))
    pieces = []
    for a in range(us):
        piece = lax.dynamic_index_in_dim(both, u ^ a, 1, keepdims=False)

        def home(i, j, a=a):
            return ((j & 1) * us + ((i % us) ^ a), (j & ~1) | (i // us))

        pieces.append(move(piece, home))
    out = call(
        functools.partial(last_kernel, layers),
        "last",
        u.astype(jnp.int32).reshape(1),
        (*pieces, (full, layers), own),
        shape((rows, width_all), BF16),
    )
    return out[None]


def solution(mesh):
    return jax.shard_map(
        per_device,
        mesh=mesh,
        in_specs=(
            P("head", "seq", None),
            P("head", None, None),
            P("head"),
            P(),
            P(),
            P(),
            P(("seq", "head"), None),
            P(("seq", "head"), None),
            P(("seq", "head"), None),
            P(("seq", "head"), None),
            P(None, ("seq", "head"), None),
            P(None, ("seq", "head"), None),
        ),
        out_specs=P("head", "seq", None),
        check_vma=False,
    )
```
